1024 devices in a mesh: dp: 4 (over y), fsdp: 256 (over z, x, core).
Axes of the slice: x: 4, y: 4, z: 32, core: 2. Of those that a mesh axis runs over, the one named last changes fastest.
Arguments:
- grad: bfloat16 [4, 8192, 14336], P('dp', 'fsdp'), may hold values from -120 to 120
- error: bfloat16 [4, 8192, 14336], P('dp', 'fsdp'), may hold values from -3 to 3
- q_init: float32 [14336, 32], replicated, may hold values from -6 to 6
Outputs:
- update: float32 [8192, 14336], P('fsdp')
- new_error: bfloat16 [4, 8192, 14336], P('dp', 'fsdp')
The draws below stay inside these ranges and needn't reach their ends.
All inputs are finite; a program needn't handle non-finite values.
Results may differ from the reference program's by a relative error of at most 0.001.
Values sent between devices are 32-bit elements; how exact they have to be, the bound alone decides.
A program may use at most 64 MiB of HBM per device.

```python
import jax
import jax.numpy as jnp
from jax import lax

D = 8192
COLS = 14336
RANK = 32
REPLICAS = 4


def draw_grad(key, part):
    first, second = jax.random.split(jax.random.fold_in(key, 17), 2)
    rows = jnp.arange(D, dtype=jnp.float32)
    row_scale = 3.0 ** (rows / D)
    col_scale = jnp.exp(jax.random.uniform(second, (COLS,), jnp.float32, 0.0, 2.302585))
    base = jnp.clip(jax.random.normal(first, (REPLICAS, D, COLS), jnp.float32), -4.0, 4.0)
    values = base * row_scale[None, :, None] * col_scale[None, None, :]
    return values.astype(jnp.bfloat16)


def block_levels(own_key, extent, shards, least, largest):
    gain = 1.0
    for axis_at, parts in shards:
        steps = jax.random.uniform(jax.random.fold_in(jax.random.fold_in(own_key, 6), axis_at), (parts,), jnp.float32, least / len(shards), largest / len(shards))
        gain = gain * jnp.repeat(jnp.exp(steps), extent[axis_at] // parts).reshape((-1,) + (1,) * (len(extent) - 1 - axis_at))
    return gain


def noise(stream_key, shape, width, reach, cuts=(), held_as=jnp.bfloat16):
    loudness = block_levels(stream_key, shape, cuts, -0.22, 0.18) if cuts else 1.0
    values = jax.random.normal(stream_key, shape, jnp.float32) * width * loudness
    return jnp.minimum(jnp.maximum(values, -reach), reach).astype(held_as)


def setup_inputs(seed: int = 0) -> dict:
    keys = jax.random.split(jax.random.key(seed), 4)
    return {
        "grad": draw_grad(jax.random.fold_in(keys[3], 71), 0),
        "error": noise(keys[1], (REPLICAS, D, COLS), 0.5, 3.0, ((0, 4), (1, 256))),
        "q_init": noise(keys[2], (COLS, RANK), 1.0, 6.0, (), jnp.float32),
    }


def reference(grad, error, q_init):

    def left_part(index):
        merged = grad[index].astype(jnp.float32) + error[index].astype(jnp.float32)
        return jnp.dot(merged, q_init, precision=lax.Precision.HIGHEST)
    p_sum = jnp.sum(lax.map(left_part, jnp.arange(REPLICAS, dtype=jnp.int32)), axis=0)
    gram = jnp.dot(p_sum.T, p_sum, precision=lax.Precision.HIGHEST)
    lower = jnp.linalg.cholesky(gram)
    p_hat = jax.scipy.linalg.solve_triangular(lower, p_sum.T, lower=True).T

    def right_part(index):
        merged = grad[index].astype(jnp.float32) + error[index].astype(jnp.float32)
        return jnp.dot(merged.T, p_hat, precision=lax.Precision.HIGHEST)
    q_mean = jnp.sum(lax.map(right_part, jnp.arange(REPLICAS, dtype=jnp.int32)), axis=0) * (1.0 / REPLICAS)
    update = jnp.dot(p_hat, q_mean.T, precision=lax.Precision.HIGHEST)

    def residual_part(index):
        merged = grad[index].astype(jnp.float32) + error[index].astype(jnp.float32)
        return (merged - update).astype(jnp.bfloat16)
    new_error = lax.map(residual_part, jnp.arange(REPLICAS, dtype=jnp.int32))
    return (update, new_error)
```

```python
import functools

import jax
import jax.numpy as jnp
from jax import lax
from jax.experimental import pallas as pl
from jax.experimental.pallas import tpu as pltpu
from jax.sharding import Mesh
from jax.sharding import PartitionSpec as P

FSDP = ("fsdp_0", "fsdp_1", "fsdp_2")
F32 = jnp.float32
BF16 = jnp.bfloat16
MESH = pl.DeviceIdType.MESH
HIGHEST = lax.Precision.HIGHEST
RANK = 32


def three_parts(v):
    hi = v.astype(BF16)
    rest = v - hi.astype(F32)
    mid = rest.astype(BF16)
    return hi, mid, (rest - mid.astype(F32)).astype(BF16)


def far_first(n):
    return sorted(range(1, n), key=lambda k: -min(k, n - k))


def kernel(
    dims, g_hbm, e_hbm, q_hbm, update_ref, error_ref,
    ge, q0, pslots, core_out, mine, core_in,
    a1, b1, a1s, b1s, a2, b2, zb, z1, f1, zfin, qfin,
    gcore, gx, gz, gf, load_sem, send, recv, hand,
):
    n, zn, far, base = dims
    pieces = 2 * n
    y, z = lax.axis_index("dp"), lax.axis_index("fsdp_0")
    x, c = lax.axis_index("fsdp_1"), lax.axis_index("fsdp_2")
    zc, zi = z // zn, z % zn
    rows = g_hbm.shape[0]
    cols = g_hbm.shape[1]
    width = cols // (2 * pieces)
    lanes = width // 128
    t2 = a2.shape[1]
    zt = z1.shape[1]
    sends = []

    def at_y(k):
        return ((y + k) % n, z, x, c)

    def at_x(k):
        return (y, z, (x + k) % n, c)

    def at_c(k):
        return (y, z, x, (c + k) % 2)

    def at_z(k):
        return (y, zc * zn + (zi + k) % zn, x, c)

    def at_far(k):
        return (y, ((zc + k) % far) * zn + zi, x, c)

    def push(name, src, dst, slot, k, peer):
        copy = pltpu.make_async_remote_copy(
            src_ref=src, dst_ref=dst,
            send_sem=send.at[base[name] + k], recv_sem=recv.at[base[name] + slot],
            device_id=peer, device_id_type=MESH,
        )
        copy.start()
        sends.append(copy)

    def arrive(name, dst, slot):
        pltpu.make_async_remote_copy(
            src_ref=dst, dst_ref=dst,
            send_sem=send.at[base[name]], recv_sem=recv.at[base[name] + slot],
            device_id=at_c(1), device_id_type=MESH,
        ).wait_recv()

    def arrive_all(name, slots, me, count):
        for k in range(1, count):
            at = (me + k) % count
            arrive(name, slots.at[at], at)

    groups = 4
    step = cols // groups
    loads = []
    for i in range(groups):
        part = pl.ds(i * step, step)
        trio = (
            (g_hbm.at[:, part], ge.at[0:rows, part]),
            (e_hbm.at[:, part], ge.at[rows : 2 * rows, part]),
            (q_hbm.at[:, part], q0.at[:, part]),
        )
        trio = [pltpu.make_async_copy(s, d, load_sem.at[i, j]) for j, (s, d) in enumerate(trio)]
        for copy in trio:
            copy.start()
        loads.append(trio)
    barrier = pltpu.get_barrier_semaphore()
    beside = sorted({1, far - 1})
    near = [at_y(k) for k in range(1, n)] + [at_x(k) for k in range(1, n)]
    near += [at_c(1)] + [at_z(k) for k in range(1, zn)] + [at_far(k) for k in beside]
    for peer in near:
        pl.semaphore_signal(barrier, inc=1, device_id=peer, device_id_type=MESH)

    if zn * zt > 2 * t2:
        zb[2 * t2 :] = jnp.zeros((zn * zt - 2 * t2, 8, 128), F32)

    acc = jnp.zeros((2 * rows, 128), F32)
    sub = step // width

    def left(i, acc):
        at = pl.ds(pl.multiple_of(i * width, 128), width)
        q = jnp.concatenate([*three_parts(q0[:, at]), jnp.zeros((RANK, width), BF16)], axis=0)
        return acc + lax.dot_general(
            ge[:, at], q, (((1,), (1,)), ((), ())), preferred_element_type=F32
        )

    for i in range(groups):
        for copy in loads[i]:
            copy.wait()
        acc = lax.fori_loop(i * sub, (i + 1) * sub, left, acc)
    lane = lax.broadcasted_iota(jnp.int32, (rows, 128), 1)
    own = acc[:rows] + acc[rows:]
    own = own + pltpu.roll(own, 96, 1) + pltpu.roll(own, 64, 1)
    pslots[y] = jnp.where(lane < RANK, own, 0.0)

    pl.semaphore_wait(barrier, len(near))
    for k in far_first(n):
        push("p", pslots.at[y], pslots.at[y], y, k, at_y(k))
    if far > 2:
        for k in beside:
            pl.semaphore_signal(hand.at[0], inc=1, device_id=at_far(k), device_id_type=MESH)
    arrive_all("p", pslots, y, n)
    p = pslots[0]
    for k in range(1, n):
        p = p + pslots[k]

    square = jnp.concatenate([p, jnp.zeros((128 - rows, 128), F32)], axis=0)
    turned = square.T[:RANK]
    gram = lax.dot_general(
        turned, square, (((1,), (0,)), ((), ())), precision=HIGHEST, preferred_element_type=F32
    )
    tile = gram[0:8]
    for a in range(1, RANK // 8):
        tile = tile + pltpu.roll(gram[8 * a : 8 * a + 8], 32 * a, 1)
    gcore[c] = tile
    push("gc", gcore.at[c], gcore.at[c], c, 0, at_c(1))

    twice = turned + pltpu.roll(turned, rows, 1)
    p3 = jnp.concatenate([*three_parts(twice)], axis=0)[:, : 2 * rows]

    def right(half, at, out):
        off = pl.multiple_of((half * pieces + at) * width, 128)
        r = lax.dot_general(
            p3, ge[:, pl.ds(off, width)], (((1,), (0,)), ((), ())), preferred_element_type=F32
        )
        r = r[:RANK] + (r[RANK : 2 * RANK] + r[2 * RANK :])
        for j in range(lanes):
            out[at, 4 * j : 4 * j + 4] = r[:, 128 * j : 128 * j + 128].reshape(4, 8, 128)

    order = []
    for k in [*far_first(n), 0]:
        order += [("a", k, (x + k) % n), ("b", k, n + (y + k) % n)]
    for s, (_, _, at) in enumerate(order):
        right((c + 1) % 2, at, core_out)
        push("cr", core_out.at[at], core_in.at[at], s, s, at_c(1))

    arrive("gc", gcore.at[(c + 1) % 2], (c + 1) % 2)
    gx[x] = gcore[0] + gcore[1]
    for k in far_first(n):
        push("gx", gx.at[x], gx.at[x], x, k, at_x(k))
    if far > 4:
        pl.semaphore_wait(hand.at[0], len(beside))
        for k in (2, far - 2):
            pl.semaphore_signal(hand.at[1], inc=1, device_id=at_far(k), device_id_type=MESH)

    for s, (kind, k, at) in enumerate(order):
        right(c, at, mine)
        arrive("cr", core_in.at[at], s)
        mine[at] = mine[at] + core_in[at]
        if k:
            if kind == "a":
                push("a1", mine.at[at], a1.at[x], x, k, at_x(k))
            else:
                push("b1", mine.at[at], b1.at[y], y, k, at_y(k))

    arrive_all("gx", gx, x, n)
    g = gx[0]
    for k in range(1, n):
        g = g + gx[k]
    gz[zi] = g
    for k in range(1, zn):
        push("gz", gz.at[zi], gz.at[zi], zi, k, at_z(k))
    arrive_all("gz", gz, zi, zn)
    g = gz[0]
    for k in range(1, zn):
        g = g + gz[k]
    gf[zc] = g
    if far > 4:
        pl.semaphore_wait(hand.at[1], 2)
    elif far > 2:
        pl.semaphore_wait(hand.at[0], len(beside))
    for k in far_first(far):
        push("gf", gf.at[zc], gf.at[zc], zc, k, at_far(k))

    def gathered(first, slots, me, count):
        total = first
        for k in range(1, count):
            total = total + slots[(me + k) % count]
        return total

    arrive_all("a1", a1, x, n)
    a1s[...] = gathered(mine[x], a1, x, n)
    for k in far_first(n):
        push("a2", a1s.at[pl.ds(((y + k) % n) * t2, t2)], a2.at[y], y, k, at_y(k))
    arrive_all("b1", b1, y, n)
    b1s[...] = gathered(mine[n + y], b1, y, n)
    for k in far_first(n):
        push("b2", b1s.at[pl.ds(((x + k) % n) * t2, t2)], b2.at[x], x, k, at_x(k))
    arrive_all("a2", a2, y, n)
    zb[0:t2] = gathered(a1s[pl.ds(y * t2, t2)], a2, y, n)
    arrive_all("b2", b2, x, n)
    zb[t2 : 2 * t2] = gathered(b1s[pl.ds(x * t2, t2)], b2, x, n)

    for k in range(1, zn):
        push("z1", zb.at[pl.ds(((zi + k) % zn) * zt, zt)], z1.at[zi], zi, k, at_z(k))
    arrive_all("z1", z1, zi, zn)
    f1[zc] = gathered(zb[pl.ds(zi * zt, zt)], z1, zi, zn)
    for k in far_first(far):
        push("f1", f1.at[zc], f1.at[zc], zc, k, at_far(k))

    arrive_all("gf", gf, zc, far)
    g = gf[0]
    for k in range(1, far):
        g = g + gf[k]
    lane = lax.broadcasted_iota(jnp.int32, (RANK, 128), 1)
    line = lax.broadcasted_iota(jnp.int32, (RANK, 128), 0)
    spread = [g] + [pltpu.roll(g, 128 - 32 * a, 1) for a in range(1, RANK // 8)]
    aug = jnp.where(lane < RANK, jnp.concatenate(spread, axis=0), 0.0)
    aug = jnp.where(lane == line + RANK, 1.0, aug)
    for k in range(RANK):
        inv = 1.0 / jnp.sqrt(aug[k : k + 1, k : k + 1])
        row = aug[k : k + 1, :] * inv
        col = aug[:, k : k + 1] * inv
        less = aug - col * row
        aug = jnp.where(line > k, less, jnp.where(line == k, row, aug))
    linv = jnp.where(lane < RANK, pltpu.roll(aug, 96, 1), 0.0)
    linv = jnp.concatenate([linv, jnp.zeros((128 - RANK, 128), F32)], axis=0)
    p_hat = lax.dot_general(
        p, linv, (((1,), (1,)), ((), ())), precision=HIGHEST, preferred_element_type=F32
    )
    w = lax.dot_general(
        p_hat, linv, (((1,), (0,)), ((), ())), precision=HIGHEST, preferred_element_type=F32
    )
    hi, mid, lo = [v.astype(F32) for v in three_parts(w * (1.0 / n))]
    w1 = hi + pltpu.roll(mid, 32, 1) + pltpu.roll(lo, 64, 1) + pltpu.roll(hi, 96, 1)
    w2 = mid + pltpu.roll(hi, 32, 1)
    w6 = jnp.concatenate([w1, w2], axis=1)[:, : 6 * RANK].astype(BF16)

    arrive_all("f1", f1, zc, far)
    total = f1[0]
    for k in range(1, far):
        total = total + f1[k]
    here = pl.ds(zi * zt, zt)
    zfin[here] = total
    for k in range(1, zn):
        push("z2", zfin.at[here], zfin.at[here], zi, k, at_z(k))
    for k in range(1, zn):
        at = (zi + k) % zn
        arrive("z2", zfin.at[pl.ds(at * zt, zt)], at)

    pa, pb = c * pieces + x, c * pieces + n + y
    part_y, part_x = pl.ds(y * t2, t2), pl.ds(x * t2, t2)
    for k in far_first(n):
        push("a3", zfin.at[0:t2], qfin.at[pa, part_y], y, k, at_y(k))
    for k in far_first(n):
        push("b3", zfin.at[t2 : 2 * t2], qfin.at[pb, part_x], x, k, at_x(k))
    qfin[pa, part_y] = zfin[0:t2]
    qfin[pb, part_x] = zfin[t2 : 2 * t2]

    def finish(at):
        q = jnp.concatenate(
            [qfin[at, 4 * j : 4 * j + 4].reshape(RANK, 128) for j in range(lanes)], axis=1
        )
        hi, mid, lo = three_parts(q)
        q6 = jnp.concatenate([hi, hi, hi, mid, mid, lo], axis=0)
        u = lax.dot_general(w6, q6, (((1,), (0,)), ((), ())), preferred_element_type=F32)
        where = pl.ds(pl.multiple_of(at * width, 128), width)
        merged = ge[0:rows, where].astype(F32) + ge[rows : 2 * rows, where].astype(F32)
        update_ref[:, where] = u
        error_ref[:, where] = (merged - u).astype(BF16)

    for k in range(1, n):
        at = (y + k) % n
        arrive("a3", qfin.at[pa, pl.ds(at * t2, t2)], at)
    for k in far_first(n):
        push("a4", qfin.at[pa], qfin.at[pa], x, k, at_x(k))
    push("cg", qfin.at[pa], qfin.at[pa], 0, 0, at_c(1))
    for k in range(1, n):
        at = (x + k) % n
        arrive("b3", qfin.at[pb, pl.ds(at * t2, t2)], at)
    for k in far_first(n):
        push("b4", qfin.at[pb], qfin.at[pb], y, k, at_y(k))
    push("cg", qfin.at[pb], qfin.at[pb], 1, 1, at_c(1))
    finish(pa)
    finish(pb)
    other = (c + 1) % 2
    turns = [x, n + y]
    for k in far_first(n):
        for name, at, slot in (
            ("a4", (x + n - k) % n, (x + n - k) % n),
            ("b4", n + (y + n - k) % n, (y + n - k) % n),
        ):
            s = len(turns)
            turns.append(at)
            at = c * pieces + at
            arrive(name, qfin.at[at], slot)
            push("cg", qfin.at[at], qfin.at[at], s, s, at_c(1))
            finish(at)
    for s, at in enumerate(turns):
        at = other * pieces + at
        arrive("cg", qfin.at[at], s)
        finish(at)
    for copy in sends:
        copy.wait_send()


def body(n, zn, far, grad, error, q_init):
    rows, cols = grad.shape[1:]
    pieces = 2 * n
    t1 = cols // (2 * pieces) // 128 * (RANK // 8)
    t2 = t1 // n
    zt = -(-2 * t2 // zn)
    base, total = {}, 0
    for name, count in (
        ("p", n), ("gc", 2), ("gx", n), ("gz", zn), ("gf", far), ("cr", pieces),
        ("a1", n), ("b1", n), ("a2", n), ("b2", n), ("z1", zn), ("f1", far), ("z2", zn),
        ("a3", n), ("b3", n), ("a4", n), ("b4", n), ("cg", pieces),
    ):
        base[name] = total
        total += count

    def tiles(*lead):
        return pltpu.VMEM((*lead, 8, 128), F32)

    vmem = pl.BlockSpec(memory_space=pltpu.VMEM)
    hbm = pl.BlockSpec(memory_space=pltpu.HBM)
    update, new_error = pl.pallas_call(
        functools.partial(kernel, (n, zn, far, base)),
        out_shape=(
            jax.ShapeDtypeStruct((rows, cols), F32),
            jax.ShapeDtypeStruct((rows, cols), BF16),
        ),
        in_specs=[hbm] * 3,
        out_specs=(vmem, vmem),
        scratch_shapes=[
            pltpu.VMEM((2 * rows, cols), BF16),
            pltpu.VMEM((RANK, cols), F32),
            pltpu.VMEM((n, rows, 128), F32),
            tiles(pieces, t1),
            tiles(pieces, t1),
            tiles(pieces, t1),
            tiles(n, t1),
            tiles(n, t1),
            tiles(t1),
            tiles(t1),
            tiles(n, t2),
            tiles(n, t2),
            tiles(zn * zt),
            tiles(zn, zt),
            tiles(far, zt),
            tiles(zn * zt),
            tiles(2 * pieces, t1),
            tiles(2),
            tiles(n),
            tiles(zn),
            tiles(far),
            pltpu.SemaphoreType.DMA((4, 3)),
            pltpu.SemaphoreType.DMA((total,)),
            pltpu.SemaphoreType.DMA((total,)),
            pltpu.SemaphoreType.REGULAR((2,)),
        ],
        compiler_params=pltpu.CompilerParams(
            collective_id=0, has_side_effects=True, vmem_limit_bytes=60 * 1024 * 1024
        ),
        name="powersgd",
    )(grad[0], error[0], q_init.T)
    return update, new_error[None]


def solution(mesh):
    n, z = mesh.shape["dp"], mesh.shape["fsdp"] // (2 * mesh.shape["dp"])
    zn = min(4, z // 2)
    split = Mesh(mesh.devices.reshape(n, z, n, 2), ("dp", *FSDP))
    placed = (P("dp", FSDP, None), P("dp", FSDP, None), P())
    return jax.shard_map(
        functools.partial(body, n, zn, z // zn),
        mesh=split,
        in_specs=placed,
        out_specs=(P(FSDP, None), P("dp", FSDP, None)),
        check_vma=False,
    )
```

```python
import functools

import jax
import jax.numpy as jnp
from jax import lax
from jax.experimental import pallas as pl
from jax.experimental.pallas import tpu as pltpu
from jax.sharding import Mesh
from jax.sharding import PartitionSpec as P

FSDP = ("fsdp_0", "fsdp_1", "fsdp_2")
F32 = jnp.float32
BF16 = jnp.bfloat16
MESH = pl.DeviceIdType.MESH
HIGHEST = lax.Precision.HIGHEST
RANK = 32
PARTS = 4
GRANT = 52200


def three_parts(v):
    hi = v.astype(BF16)
    rest = v - hi.astype(F32)
    mid = rest.astype(BF16)
    return hi, mid, (rest - mid.astype(F32)).astype(BF16)


def far_first(n):
    return sorted(range(1, n), key=lambda k: -min(k, n - k))


def pack(v):
    tile = v[0:8]
    for a in range(1, RANK // 8):
        tile = tile + pltpu.roll(v[8 * a : 8 * a + 8], RANK * a, 1)
    return tile


def unpack(tile):
    spread = [tile] + [pltpu.roll(tile, 128 - RANK * a, 1) for a in range(1, RANK // 8)]
    lane = lax.broadcasted_iota(jnp.int32, (RANK, 128), 1)
    return jnp.where(lane < RANK, jnp.concatenate(spread, axis=0), 0.0)


def kernel(
    dims, g_hbm, e_hbm, q_hbm, *refs
):
    n, zn, far, base, parts = dims
    update_refs, error_ref, refs = refs[:parts], refs[parts], refs[parts + 1 :]
    (
        ge, q0, pslots, core_out, mine, core_in,
        a1, b1, a1s, b1s, a2, b2, f1, zfin, afin, bfin, qfin,
        gcore, gx, gz, gf, load_sem, send, recv, hand,
    ) = refs
    pieces = 2 * n
    y, z = lax.axis_index("dp"), lax.axis_index("fsdp_0")
    x, c = lax.axis_index("fsdp_1"), lax.axis_index("fsdp_2")
    zc, zi = z // zn, z % zn
    rows = g_hbm.shape[0]
    cols = g_hbm.shape[1]
    width = cols // (2 * pieces)
    lanes = width // 128
    t1 = mine.shape[1]
    t2 = t1 // n
    t3 = a2.shape[2]
    sends = []
    sent = iter(range(send.shape[0]))

    def at(dy=0, dx=0, dc=0, dz=0, df=0):
        to_y = (y + dy) % n if dy else y
        to_x = (x + dx) % n if dx else x
        to_c = (c + dc) % 2 if dc else c
        to_zi = (zi + dz) % zn if dz else zi
        to_zc = (zc + df) % far if df else zc
        return (to_y, to_zc * zn + to_zi, to_x, to_c)

    def push(name, src, dst, slot, peer):
        copy = pltpu.make_async_remote_copy(
            src_ref=src, dst_ref=dst,
            send_sem=send.at[next(sent)], recv_sem=recv.at[base[name] + slot],
            device_id=peer, device_id_type=MESH,
        )
        copy.start()
        sends.append(copy)

    def arrive(name, dst, slot):
        pltpu.make_async_remote_copy(
            src_ref=dst, dst_ref=dst,
            send_sem=send.at[0], recv_sem=recv.at[base[name] + slot],
            device_id=at(dc=1), device_id_type=MESH,
        ).wait_recv()

    def arrive_all(name, slots, me, count):
        for k in range(1, count):
            src = (me + k) % count
            arrive(name, slots.at[src], src)

    groups = 4
    step = cols // groups
    loads = []
    for i in range(groups):
        part = pl.ds(i * step, step)
        trio = (
            (g_hbm.at[:, part], ge.at[0:rows, part]),
            (e_hbm.at[:, part], ge.at[rows : 2 * rows, part]),
            (q_hbm.at[:, part], q0.at[:, part]),
        )
        trio = [pltpu.make_async_copy(s, d, load_sem.at[i, j]) for j, (s, d) in enumerate(trio)]
        for copy in trio:
            copy.start()
        loads.append(trio)
    barrier = pltpu.get_barrier_semaphore()
    beside = sorted({1, far - 1})
    near = [at(dy=k, dz=m) for m in range(zn) for k in range(n) if k or m]
    near += [at(dx=k, dz=m) for m in range(zn) for k in range(1, n)]
    near += [at(dc=1)] + [at(df=k) for k in beside]
    for peer in near:
        pl.semaphore_signal(barrier, inc=1, device_id=peer, device_id_type=MESH)

    for k in range(n if zn * t3 > t2 else 0):
        a1s[k, t2:] = jnp.zeros((zn * t3 - t2, 8, 128), F32)
        b1s[k, t2:] = jnp.zeros((zn * t3 - t2, 8, 128), F32)

    acc = jnp.zeros((2 * rows, 128), F32)
    sub = step // width

    def left(i, acc):
        where = pl.ds(pl.multiple_of(i * width, 128), width)
        q = jnp.concatenate([*three_parts(q0[:, where]), jnp.zeros((RANK, width), BF16)], axis=0)
        return acc + lax.dot_general(
            ge[:, where], q, (((1,), (1,)), ((), ())), preferred_element_type=F32
        )

    for i in range(groups):
        for copy in loads[i]:
            copy.wait()
        acc = lax.fori_loop(i * sub, (i + 1) * sub, left, acc)
    lane = lax.broadcasted_iota(jnp.int32, (rows, 128), 1)
    own = acc[:rows] + acc[rows:]
    own = own + pltpu.roll(own, 96, 1) + pltpu.roll(own, 64, 1)
    pslots[y] = pack(jnp.where(lane < RANK, own, 0.0))

    pl.semaphore_wait(barrier, len(near))
    for k in far_first(n):
        push("p", pslots.at[y], pslots.at[y], y, at(dy=k))
    if far > 2:
        for k in beside:
            pl.semaphore_signal(hand.at[0], inc=1, device_id=at(df=k), device_id_type=MESH)
    arrive_all("p", pslots, y, n)
    p = pslots[0]
    for k in range(1, n):
        p = p + pslots[k]
    p = unpack(p)

    square = jnp.concatenate([p, jnp.zeros((128 - rows, 128), F32)], axis=0)
    turned = square.T[:RANK]
    gram = lax.dot_general(
        turned, square, (((1,), (0,)), ((), ())), precision=HIGHEST, preferred_element_type=F32
    )
    gcore[c] = pack(gram)
    push("gc", gcore.at[c], gcore.at[c], c, at(dc=1))

    twice = turned + pltpu.roll(turned, rows, 1)
    p3 = jnp.concatenate([*three_parts(twice)], axis=0)[:, : 2 * rows]

    def right(half, piece):
        off = pl.multiple_of((half * pieces + piece) * width, 128)
        r = lax.dot_general(
            p3, ge[:, pl.ds(off, width)], (((1,), (0,)), ((), ())), preferred_element_type=F32
        )
        r = r[:RANK] + (r[RANK : 2 * RANK] + r[2 * RANK :])
        return [r[:, 128 * j : 128 * j + 128].reshape(4, 8, 128) for j in range(lanes)]

    order = []
    for k in [*far_first(n), 0]:
        order += [("a", k, (x + k) % n), ("b", k, n + (y + k) % n)]
    turn = [*far_first(n), 0]

    def first_stage(kind, k, piece, group):
        if kind == "a":
            g = (y + group) % n
            part = pl.ds(g * t2, t2)
            push("a1", mine.at[piece, part], a1.at[x, part], x * n + g, at(dx=k))
        else:
            g = (x + group) % n
            part = pl.ds(g * t2, t2)
            push("b1", mine.at[piece, part], b1.at[y, part], y * n + g, at(dy=k))

    ahead = 3
    for s in range(len(order) + ahead):
        if s < len(order):
            piece = order[s][2]
            for j, tile in enumerate(right((c + 1) % 2, piece)):
                core_out[piece, 4 * j : 4 * j + 4] = tile
            push("cr", core_out.at[piece], core_in.at[piece], s, at(dc=1))
        if s == 5:
            arrive("gc", gcore.at[(c + 1) % 2], (c + 1) % 2)
            gx[x] = gcore[0] + gcore[1]
            for k in far_first(n):
                push("gx", gx.at[x], gx.at[x], x, at(dx=k))
            if far > 4:
                pl.semaphore_wait(hand.at[0], len(beside))
                for k in (2, far - 2):
                    pl.semaphore_signal(
                        hand.at[1], inc=1, device_id=at(df=k), device_id_type=MESH
                    )
        if s >= ahead:
            kind, k, piece = order[s - ahead]
            tiles = right(c, piece)
            arrive("cr", core_in.at[piece], s - ahead)
            for j, tile in enumerate(tiles):
                part = slice(4 * j, 4 * j + 4)
                mine[piece, part] = tile + core_in[piece, part]
            if k:
                for group in turn[: n // 2]:
                    first_stage(kind, k, piece, group)
    for group in turn[n // 2 :]:
        for kind, k, piece in order:
            if k:
                first_stage(kind, k, piece, group)

    arrive_all("gx", gx, x, n)
    g = gx[0]
    for k in range(1, n):
        g = g + gx[k]
    gz[zi] = g
    for k in range(1, zn):
        push("gz", gz.at[zi], gz.at[zi], zi, at(dz=k))

    for group in turn:
        for kind in ("a", "b"):
            if kind == "a":
                me, other, slots, sums, piece = x, y, a1, a1s, x
            else:
                me, other, slots, sums, piece = y, x, b1, b1s, n + y
            g = (other + group) % n
            part = pl.ds(g * t2, t2)
            total = mine[piece, part]
            for k in range(1, n):
                src = (me + k) % n
                arrive(kind + "1", slots.at[src, part], src * n + g)
                total = total + slots[src, part]
            sums[g, 0:t2] = total
            for m in range(zn):
                if group == 0 and m == 0:
                    continue
                chunk = sums.at[g, pl.ds(((zi + m) % zn) * t3, t3)]
                slot = other * zn + zi
                if kind == "a":
                    push("a2", chunk, a2.at[y, zi], slot, at(dy=group, dz=m))
                else:
                    push("b2", chunk, b2.at[x, zi], slot, at(dx=group, dz=m))

    arrive_all("gz", gz, zi, zn)
    g = gz[0]
    for k in range(1, zn):
        g = g + gz[k]
    gf[zc] = g
    if far > 4:
        pl.semaphore_wait(hand.at[1], 2)
    elif far > 2:
        pl.semaphore_wait(hand.at[0], len(beside))
    for k in far_first(far):
        push("gf", gf.at[zc], gf.at[zc], zc, at(df=k))

    own_part = pl.ds(zi * t3, t3)
    for kind in ("a", "b"):
        other, slots, sums = (y, a2, a1s) if kind == "a" else (x, b2, b1s)
        total = sums[other, own_part]
        for group in [0, *far_first(n)[::-1]]:
            for m in range(zn):
                if group == 0 and m == 0:
                    continue
                o, i = (other + group) % n, (zi + m) % zn
                arrive(kind + "2", slots.at[o, i], o * zn + i)
                total = total + slots[o, i]
        if kind == "a":
            f1[zc, 0:t3] = total
        else:
            f1[zc, t3:] = total

    for k in far_first(far):
        push("f1", f1.at[zc], f1.at[zc], zc, at(df=k))

    arrive_all("gf", gf, zc, far)
    g = gf[0]
    for k in range(1, far):
        g = g + gf[k]
    lane = lax.broadcasted_iota(jnp.int32, (RANK, 128), 1)
    line = lax.broadcasted_iota(jnp.int32, (RANK, 128), 0)
    aug = jnp.where(lane == line + RANK, 1.0, unpack(g))
    for k in range(RANK):
        inv = 1.0 / jnp.sqrt(aug[k : k + 1, k : k + 1])
        row = aug[k : k + 1, :] * inv
        col = aug[:, k : k + 1] * inv
        less = aug - col * row
        aug = jnp.where(line > k, less, jnp.where(line == k, row, aug))
    linv = jnp.where(lane < RANK, pltpu.roll(aug, 96, 1), 0.0)
    linv = jnp.concatenate([linv, jnp.zeros((128 - RANK, 128), F32)], axis=0)
    p_hat = lax.dot_general(
        p, linv, (((1,), (1,)), ((), ())), precision=HIGHEST, preferred_element_type=F32
    )
    w = lax.dot_general(
        p_hat, linv, (((1,), (0,)), ((), ())), precision=HIGHEST, preferred_element_type=F32
    )
    hi, mid, lo = [v.astype(F32) for v in three_parts(w * (1.0 / n))]
    w1 = hi + pltpu.roll(mid, 32, 1) + pltpu.roll(lo, 64, 1) + pltpu.roll(hi, 96, 1)
    w2 = mid + pltpu.roll(hi, 32, 1)
    w6 = jnp.concatenate([w1, w2], axis=1)[:, : 6 * RANK].astype(BF16)

    arrive_all("f1", f1, zc, far)
    total = f1[0]
    for k in range(1, far):
        total = total + f1[k]
    zfin[...] = total

    for group in turn:
        for m in range(zn):
            if group == 0 and m == 0:
                continue
            slot = zi + zn * y
            push("a3", zfin.at[0:t3], afin.at[y, own_part], slot, at(dy=group, dz=m))
            slot = zi + zn * x
            push("b3", zfin.at[t3 : 2 * t3], bfin.at[x, own_part], slot, at(dx=group, dz=m))
    afin[y, own_part] = total[:t3]
    bfin[x, own_part] = total[t3:]

    def finish(piece):
        q = jnp.concatenate(
            [qfin[piece, 4 * j : 4 * j + 4].reshape(RANK, 128) for j in range(lanes)], axis=1
        )
        hi, mid, lo = three_parts(q)
        q6 = jnp.concatenate([hi, hi, hi, mid, mid, lo], axis=0)
        u = lax.dot_general(w6, q6, (((1,), (0,)), ((), ())), preferred_element_type=F32)
        where = pl.ds(pl.multiple_of(piece * width, 128), width)
        merged = ge[0:rows, where].astype(F32) + ge[rows : 2 * rows, where].astype(F32)
        lines = rows // parts
        for i in range(parts):
            update_refs[i][:, where] = u[i * lines : i * lines + lines]
        error_ref[:, where] = (merged - u).astype(BF16)

    pa, pb = c * pieces + x, c * pieces + n + y
    for group in turn[::-1]:
        for kind in ("a", "b"):
            other, slots, piece = (y, afin, pa) if kind == "a" else (x, bfin, pb)
            g = (other + group) % n
            for m in range(zn):
                if group == 0 and m == 0:
                    continue
                i = (zi + m) % zn
                arrive(kind + "3", slots.at[g, pl.ds(i * t3, t3)], g * zn + i)
            part = pl.ds(g * t2, t2)
            for k in far_first(n):
                if kind == "a":
                    push("a4", afin.at[g, 0:t2], qfin.at[pa, part], x * n + g, at(dx=k))
                else:
                    push("b4", bfin.at[g, 0:t2], qfin.at[pb, part], y * n + g, at(dy=k))
            slot = (0 if kind == "a" else n) + g
            push("cg", slots.at[g, 0:t2], qfin.at[piece, part], slot, at(dc=1))
            qfin[piece, part] = slots[g, 0:t2]

    finish(pa)
    finish(pb)
    half = c * pieces
    turns = []
    for k in far_first(n):
        for name, src, piece in (
            ("a4", (x + n - k) % n, (x + n - k) % n),
            ("b4", (y + n - k) % n, n + (y + n - k) % n),
        ):
            for group in turn[::-1]:
                g = ((y if name == "a4" else x) + group) % n
                arrive(name, qfin.at[half + piece, pl.ds(g * t2, t2)], src * n + g)
            push("ch", qfin.at[half + piece], qfin.at[half + piece], len(turns), at(dc=1))
            turns.append(piece)
            finish(half + piece)
    half = ((c + 1) % 2) * pieces
    for piece, slot in ((x, 0), (n + y, n)):
        for g in range(n):
            arrive("cg", qfin.at[half + piece, g * t2 : g * t2 + t2], slot + g)
        finish(half + piece)
    for s, piece in enumerate(turns):
        arrive("ch", qfin.at[half + piece], s)
        finish(half + piece)
    for copy in sends:
        copy.wait_send()


def body(n, zn, far, grad, error, q_init):
    rows, cols = grad.shape[1:]
    pieces = 2 * n
    t1 = cols // (2 * pieces) // 128 * (RANK // 8)
    t2 = t1 // n
    t3 = -(-t2 // zn)
    base, total = {}, 0
    for name, count in (
        ("p", n), ("gc", 2), ("gx", n), ("gz", zn), ("gf", far), ("cr", pieces),
        ("a1", n * n), ("b1", n * n), ("a2", n * zn), ("b2", n * zn), ("f1", far),
        ("a3", n * zn), ("b3", n * zn), ("a4", n * n), ("b4", n * n),
        ("cg", pieces), ("ch", pieces),
    ):
        base[name] = total
        total += count

    def tiles(*lead):
        return pltpu.VMEM((*lead, 8, 128), F32)

    vmem = pl.BlockSpec(memory_space=pltpu.VMEM)
    hbm = pl.BlockSpec(memory_space=pltpu.HBM)
    parts = PARTS
    *update, new_error = pl.pallas_call(
        functools.partial(kernel, (n, zn, far, base, parts)),
        out_shape=(
            *[jax.ShapeDtypeStruct((rows // parts, cols), F32)] * parts,
            jax.ShapeDtypeStruct((rows, cols), BF16),
        ),
        in_specs=[hbm] * 3,
        out_specs=(vmem,) * (parts + 1),
        scratch_shapes=[
            pltpu.VMEM((2 * rows, cols), BF16),
            pltpu.VMEM((RANK, cols), F32),
            tiles(n),
            tiles(pieces, t1),
            tiles(pieces, t1),
            tiles(pieces, t1),
            tiles(n, t1),
            tiles(n, t1),
            tiles(n, zn * t3),
            tiles(n, zn * t3),
            tiles(n, zn, t3),
            tiles(n, zn, t3),
            tiles(far, 2 * t3),
            tiles(2 * t3),
            tiles(n, zn * t3),
            tiles(n, zn * t3),
            tiles(2 * pieces, t1),
            tiles(2),
            tiles(n),
            tiles(zn),
            tiles(far),
            pltpu.SemaphoreType.DMA((4, 3)),
            pltpu.SemaphoreType.DMA((total,)),
            pltpu.SemaphoreType.DMA((total,)),
            pltpu.SemaphoreType.REGULAR((2,)),
        ],
        compiler_params=pltpu.CompilerParams(
            collective_id=0, has_side_effects=True, vmem_limit_bytes=GRANT * 1024
        ),
        name="powersgd",
    )(grad[0], error[0], q_init.T)
    return jnp.concatenate(update, axis=0), new_error[None]


def solution(mesh):
    n, z = mesh.shape["dp"], mesh.shape["fsdp"] // (2 * mesh.shape["dp"])
    zn = min(4, z // 2)
    split = Mesh(mesh.devices.reshape(n, z, n, 2), ("dp", *FSDP))
    placed = (P("dp", FSDP, None), P("dp", FSDP, None), P())
    return jax.shard_map(
        functools.partial(body, n, zn, z // zn),
        mesh=split,
        in_specs=placed,
        out_specs=(P(FSDP, None), P("dp", FSDP, None)),
        check_vma=False,
    )
```

```python
import functools

import jax
import jax.numpy as jnp
from jax import lax
from jax.experimental import pallas as pl
from jax.experimental.pallas import tpu as pltpu
from jax.sharding import Mesh
from jax.sharding import PartitionSpec as P

FSDP = ("fsdp_0", "fsdp_1", "fsdp_2")
F32 = jnp.float32
BF16 = jnp.bfloat16
MESH = pl.DeviceIdType.MESH
HIGHEST = lax.Precision.HIGHEST
RANK = 32
PARTS = 4
GRANT = 52200


def three_parts(v):
    hi = v.astype(BF16)
    rest = v - hi.astype(F32)
    mid = rest.astype(BF16)
    return hi, mid, (rest - mid.astype(F32)).astype(BF16)


def far_first(n):
    return sorted(range(1, n), key=lambda k: -min(k, n - k))


def pack(v):
    tile = v[0:8]
    for a in range(1, RANK // 8):
        tile = tile + pltpu.roll(v[8 * a : 8 * a + 8], RANK * a, 1)
    return tile


def unpack(tile):
    spread = [tile] + [pltpu.roll(tile, 128 - RANK * a, 1) for a in range(1, RANK // 8)]
    lane = lax.broadcasted_iota(jnp.int32, (RANK, 128), 1)
    return jnp.where(lane < RANK, jnp.concatenate(spread, axis=0), 0.0)


def kernel(
    dims, g_hbm, e_hbm, q_hbm, *refs
):
    n, zn, far, base, parts = dims
    update_refs, error_ref, refs = refs[:parts], refs[parts], refs[parts + 1 :]
    (
        ge, q0, pslots, core_out, mine, core_in,
        a1, b1, a1s, b1s, a2, b2, f1, zfin, afin, bfin, qfin,
        gcore, gx, gf, load_sem, send, recv, hand,
    ) = refs
    pieces = 2 * n
    y, z = lax.axis_index("dp"), lax.axis_index("fsdp_0")
    x, c = lax.axis_index("fsdp_1"), lax.axis_index("fsdp_2")
    zc, zi = z // zn, z % zn
    rows = g_hbm.shape[0]
    cols = g_hbm.shape[1]
    width = cols // (2 * pieces)
    lanes = width // 128
    t1 = mine.shape[1]
    t2 = t1 // n
    t3 = a2.shape[2]
    sends = []
    sent = iter(range(send.shape[0]))

    def at(dy=0, dx=0, dc=0, dz=0, df=0):
        to_y = (y + dy) % n if dy else y
        to_x = (x + dx) % n if dx else x
        to_c = (c + dc) % 2 if dc else c
        to_zi = (zi + dz) % zn if dz else zi
        to_zc = (zc + df) % far if df else zc
        return (to_y, to_zc * zn + to_zi, to_x, to_c)

    def push(name, src, dst, slot, peer):
        copy = pltpu.make_async_remote_copy(
            src_ref=src, dst_ref=dst,
            send_sem=send.at[next(sent)], recv_sem=recv.at[base[name] + slot],
            device_id=peer, device_id_type=MESH,
        )
        copy.start()
        sends.append(copy)

    def arrive(name, dst, slot):
        pltpu.make_async_remote_copy(
            src_ref=dst, dst_ref=dst,
            send_sem=send.at[0], recv_sem=recv.at[base[name] + slot],
            device_id=at(dc=1), device_id_type=MESH,
        ).wait_recv()

    def arrive_all(name, slots, me, count):
        for k in range(1, count):
            src = (me + k) % count
            arrive(name, slots.at[src], src)

    groups = 4
    step = cols // groups
    loads = []
    for i in range(groups):
        part = pl.ds(i * step, step)
        trio = (
            (g_hbm.at[:, part], ge.at[0:rows, part]),
            (e_hbm.at[:, part], ge.at[rows : 2 * rows, part]),
            (q_hbm.at[:, part], q0.at[:, part]),
        )
        trio = [pltpu.make_async_copy(s, d, load_sem.at[i, j]) for j, (s, d) in enumerate(trio)]
        for copy in trio:
            copy.start()
        loads.append(trio)
    barrier = pltpu.get_barrier_semaphore()
    beside = sorted({1, far - 1})
    near = [at(dy=k, dz=m) for m in range(zn) for k in range(n) if k or m]
    near += [at(dx=k, dz=m) for m in range(zn) for k in range(1, n)]
    near += [at(dc=1)] + [at(df=k) for k in beside]
    for peer in near:
        pl.semaphore_signal(barrier, inc=1, device_id=peer, device_id_type=MESH)

    for k in range(n if zn * t3 > t2 else 0):
        a1s[k, t2:] = jnp.zeros((zn * t3 - t2, 8, 128), F32)
        b1s[k, t2:] = jnp.zeros((zn * t3 - t2, 8, 128), F32)

    acc = jnp.zeros((2 * rows, 128), F32)
    sub = step // 2
    for i in range(groups):
        for copy in loads[i]:
            copy.wait()
        for j in range(i * step, (i + 1) * step, sub):
            q = [*three_parts(q0[:, j : j + sub]), jnp.zeros((RANK, sub), BF16)]
            acc = acc + lax.dot_general(
                ge[:, j : j + sub], jnp.concatenate(q, axis=0),
                (((1,), (1,)), ((), ())), preferred_element_type=F32,
            )
    lane = lax.broadcasted_iota(jnp.int32, (rows, 128), 1)
    own = acc[:rows] + acc[rows:]
    own = own + pltpu.roll(own, 96, 1) + pltpu.roll(own, 64, 1)
    pslots[y] = pack(jnp.where(lane < RANK, own, 0.0))

    pl.semaphore_wait(barrier, len(near))
    for k in far_first(n):
        push("p", pslots.at[y], pslots.at[y], y, at(dy=k))
    if far > 2:
        for k in beside:
            pl.semaphore_signal(hand.at[0], inc=1, device_id=at(df=k), device_id_type=MESH)
    arrive_all("p", pslots, y, n)
    p = pslots[0]
    for k in range(1, n):
        p = p + pslots[k]
    p = unpack(p)

    square = jnp.concatenate([p, jnp.zeros((128 - rows, 128), F32)], axis=0)
    turned = square.T[:RANK]
    gram = lax.dot_general(
        turned, square, (((1,), (0,)), ((), ())), precision=HIGHEST, preferred_element_type=F32
    )
    gcore[c] = pack(gram)
    push("gc", gcore.at[c], gcore.at[c], c, at(dc=1))

    twice = turned + pltpu.roll(turned, rows, 1)
    p3 = jnp.concatenate([*three_parts(twice)], axis=0)[:, : 2 * rows]

    def right(half, piece):
        off = pl.multiple_of((half * pieces + piece) * width, 128)
        r = lax.dot_general(
            p3, ge[:, pl.ds(off, width)], (((1,), (0,)), ((), ())), preferred_element_type=F32
        )
        r = r[:RANK] + (r[RANK : 2 * RANK] + r[2 * RANK :])
        return [r[:, 128 * j : 128 * j + 128].reshape(4, 8, 128) for j in range(lanes)]

    order = []
    for k in [*far_first(n), 0]:
        order += [("a", k, (x + k) % n), ("b", k, n + (y + k) % n)]
    turn = [*far_first(n), 0]

    def first_stage(kind, k, piece, group):
        if kind == "a":
            g = (y + group) % n
            part = pl.ds(g * t2, t2)
            push("a1", mine.at[piece, part], a1.at[x, part], x * n + g, at(dx=k))
        else:
            g = (x + group) % n
            part = pl.ds(g * t2, t2)
            push("b1", mine.at[piece, part], b1.at[y, part], y * n + g, at(dy=k))

    ahead = 3
    for s in range(len(order) + ahead):
        if s < len(order):
            piece = order[s][2]
            for j, tile in enumerate(right((c + 1) % 2, piece)):
                core_out[piece, 4 * j : 4 * j + 4] = tile
            push("cr", core_out.at[piece], core_in.at[piece], s, at(dc=1))
        if s == 4:
            arrive("gc", gcore.at[(c + 1) % 2], (c + 1) % 2)
            gx[x, zi] = gcore[0] + gcore[1]
            for k in turn:
                for m in range(zn):
                    if k or m:
                        push("gx", gx.at[x, zi], gx.at[x, zi], x * zn + zi, at(dx=k, dz=m))
            if far > 4:
                pl.semaphore_wait(hand.at[0], len(beside))
                for k in (2, far - 2):
                    pl.semaphore_signal(
                        hand.at[1], inc=1, device_id=at(df=k), device_id_type=MESH
                    )
        if s >= ahead:
            kind, k, piece = order[s - ahead]
            tiles = right(c, piece)
            arrive("cr", core_in.at[piece], s - ahead)
            for j, tile in enumerate(tiles):
                part = slice(4 * j, 4 * j + 4)
                mine[piece, part] = tile + core_in[piece, part]
            if k:
                for group in turn[: n // 2]:
                    first_stage(kind, k, piece, group)
            if s - ahead == 2 * (n - 1) - 1:
                for group in turn[n // 2 :]:
                    for entry in order[: 2 * (n - 1)]:
                        first_stage(*entry, group)

    def gram_far():
        for k in range(n):
            for m in range(zn):
                if k or m:
                    i, j = (x + k) % n, (zi + m) % zn
                    arrive("gx", gx.at[i, j], i * zn + j)
        total = gx[0, 0]
        for i in range(1, n * zn):
            total = total + gx[i // zn, i % zn]
        gf[zc] = total
        if far > 4:
            pl.semaphore_wait(hand.at[1], 2)
        elif far > 2:
            pl.semaphore_wait(hand.at[0], len(beside))
        for k in far_first(far):
            push("gf", gf.at[zc], gf.at[zc], zc, at(df=k))

    for group in turn:
        if group == turn[n // 2]:
            gram_far()
        for kind in ("a", "b"):
            if kind == "a":
                me, other, slots, sums, piece = x, y, a1, a1s, x
            else:
                me, other, slots, sums, piece = y, x, b1, b1s, n + y
            g = (other + group) % n
            part = pl.ds(g * t2, t2)
            total = mine[piece, part]
            for k in range(1, n):
                src = (me + k) % n
                arrive(kind + "1", slots.at[src, part], src * n + g)
                total = total + slots[src, part]
            sums[g, 0:t2] = total
            for m in range(zn):
                if group == 0 and m == 0:
                    continue
                chunk = sums.at[g, pl.ds(((zi + m) % zn) * t3, t3)]
                slot = other * zn + zi
                if kind == "a":
                    push("a2", chunk, a2.at[y, zi], slot, at(dy=group, dz=m))
                else:
                    push("b2", chunk, b2.at[x, zi], slot, at(dx=group, dz=m))

    own_part = pl.ds(zi * t3, t3)
    for kind in ("a", "b"):
        other, slots, sums = (y, a2, a1s) if kind == "a" else (x, b2, b1s)
        total = sums[other, own_part]
        for group in [0, *far_first(n)[::-1]]:
            for m in range(zn):
                if group == 0 and m == 0:
                    continue
                o, i = (other + group) % n, (zi + m) % zn
                arrive(kind + "2", slots.at[o, i], o * zn + i)
                total = total + slots[o, i]
        if kind == "a":
            f1[zc, 0:t3] = total
        else:
            f1[zc, t3:] = total

    for k in far_first(far):
        push("f1", f1.at[zc], f1.at[zc], zc, at(df=k))

    arrive_all("gf", gf, zc, far)
    g = gf[0]
    for k in range(1, far):
        g = g + gf[k]
    lane = lax.broadcasted_iota(jnp.int32, (RANK, 128), 1)
    line = lax.broadcasted_iota(jnp.int32, (RANK, 128), 0)
    aug = jnp.where(lane == line + RANK, 1.0, unpack(g))
    for k in range(RANK):
        inv = 1.0 / jnp.sqrt(aug[k : k + 1, k : k + 1])
        row = aug[k : k + 1, :] * inv
        col = aug[:, k : k + 1] * inv
        less = aug - col * row
        aug = jnp.where(line > k, less, jnp.where(line == k, row, aug))
    linv = jnp.where(lane < RANK, pltpu.roll(aug, 96, 1), 0.0)
    linv = jnp.concatenate([linv, jnp.zeros((128 - RANK, 128), F32)], axis=0)
    p_hat = lax.dot_general(
        p, linv, (((1,), (1,)), ((), ())), precision=HIGHEST, preferred_element_type=F32
    )
    w = lax.dot_general(
        p_hat, linv, (((1,), (0,)), ((), ())), precision=HIGHEST, preferred_element_type=F32
    )
    hi, mid, lo = [v.astype(F32) for v in three_parts(w * (1.0 / n))]
    w1 = hi + pltpu.roll(mid, 32, 1) + pltpu.roll(lo, 64, 1) + pltpu.roll(hi, 96, 1)
    w2 = mid + pltpu.roll(hi, 32, 1)
    w6 = jnp.concatenate([w1, w2], axis=1)[:, : 6 * RANK].astype(BF16)

    arrive_all("f1", f1, zc, far)
    total = f1[0]
    for k in range(1, far):
        total = total + f1[k]
    zfin[...] = total

    for group in turn[::-1]:
        for m in range(zn):
            if group == 0 and m == 0:
                continue
            slot = zi + zn * y
            push("a3", zfin.at[0:t3], afin.at[y, own_part], slot, at(dy=group, dz=m))
            slot = zi + zn * x
            push("b3", zfin.at[t3 : 2 * t3], bfin.at[x, own_part], slot, at(dx=group, dz=m))
    afin[y, own_part] = total[:t3]
    bfin[x, own_part] = total[t3:]

    def finish(piece):
        q = jnp.concatenate(
            [qfin[piece, 4 * j : 4 * j + 4].reshape(RANK, 128) for j in range(lanes)], axis=1
        )
        hi, mid, lo = three_parts(q)
        q6 = jnp.concatenate([hi, hi, hi, mid, mid, lo], axis=0)
        u = lax.dot_general(w6, q6, (((1,), (0,)), ((), ())), preferred_element_type=F32)
        where = pl.ds(pl.multiple_of(piece * width, 128), width)
        merged = ge[0:rows, where].astype(F32) + ge[rows : 2 * rows, where].astype(F32)
        lines = rows // parts
        for i in range(parts):
            update_refs[i][:, where] = u[i * lines : i * lines + lines]
        error_ref[:, where] = (merged - u).astype(BF16)

    pa, pb = c * pieces + x, c * pieces + n + y
    for group in turn[::-1]:
        for kind in ("a", "b"):
            other, slots, piece = (y, afin, pa) if kind == "a" else (x, bfin, pb)
            g = (other + group) % n
            for m in range(zn):
                if group == 0 and m == 0:
                    continue
                i = (zi + m) % zn
                arrive(kind + "3", slots.at[g, pl.ds(i * t3, t3)], g * zn + i)
            part = pl.ds(g * t2, t2)
            for k in far_first(n):
                if kind == "a":
                    push("a4", afin.at[g, 0:t2], qfin.at[pa, part], x * n + g, at(dx=k))
                else:
                    push("b4", bfin.at[g, 0:t2], qfin.at[pb, part], y * n + g, at(dy=k))
            slot = (0 if kind == "a" else n) + g
            push("cg", slots.at[g, 0:t2], qfin.at[piece, part], slot, at(dc=1))
            qfin[piece, part] = slots[g, 0:t2]

    finish(pa)
    finish(pb)
    half = c * pieces
    turns = []
    for k in far_first(n):
        for name, src, piece in (
            ("a4", (x + n - k) % n, (x + n - k) % n),
            ("b4", (y + n - k) % n, n + (y + n - k) % n),
        ):
            for group in turn[::-1]:
                g = ((y if name == "a4" else x) + group) % n
                arrive(name, qfin.at[half + piece, pl.ds(g * t2, t2)], src * n + g)
            push("ch", qfin.at[half + piece], qfin.at[half + piece], len(turns), at(dc=1))
            turns.append(piece)
            finish(half + piece)
    half = ((c + 1) % 2) * pieces
    for piece, slot in ((x, 0), (n + y, n)):
        for g in range(n):
            arrive("cg", qfin.at[half + piece, g * t2 : g * t2 + t2], slot + g)
        finish(half + piece)
    for s, piece in enumerate(turns):
        arrive("ch", qfin.at[half + piece], s)
        finish(half + piece)
    for copy in sends:
        copy.wait_send()


def write_out(*refs):
    *parts, error, whole, rounded, sem = refs
    lines = parts[0].shape[0]
    copies = [
        pltpu.make_async_copy(part, whole.at[i * lines : i * lines + lines], sem.at[i])
        for i, part in enumerate(parts)
    ]
    copies.append(pltpu.make_async_copy(error, rounded, sem.at[len(parts)]))
    for copy in copies:
        copy.start()
    for copy in copies:
        copy.wait()


def body(n, zn, far, grad, error, q_init):
    rows, cols = grad.shape[1:]
    pieces = 2 * n
    t1 = cols // (2 * pieces) // 128 * (RANK // 8)
    t2 = t1 // n
    t3 = -(-t2 // zn)
    base, total = {}, 0
    for name, count in (
        ("p", n), ("gc", 2), ("gx", n * zn), ("gf", far), ("cr", pieces),
        ("a1", n * n), ("b1", n * n), ("a2", n * zn), ("b2", n * zn), ("f1", far),
        ("a3", n * zn), ("b3", n * zn), ("a4", n * n), ("b4", n * n),
        ("cg", pieces), ("ch", pieces),
    ):
        base[name] = total
        total += count

    def tiles(*lead):
        return pltpu.VMEM((*lead, 8, 128), F32)

    vmem = pl.BlockSpec(memory_space=pltpu.VMEM)
    hbm = pl.BlockSpec(memory_space=pltpu.HBM)
    parts = PARTS
    *update, new_error = pl.pallas_call(
        functools.partial(kernel, (n, zn, far, base, parts)),
        out_shape=(
            *[jax.ShapeDtypeStruct((rows // parts, cols), F32)] * parts,
            jax.ShapeDtypeStruct((rows, cols), BF16),
        ),
        in_specs=[hbm] * 3,
        out_specs=(vmem,) * (parts + 1),
        scratch_shapes=[
            pltpu.VMEM((2 * rows, cols), BF16),
            pltpu.VMEM((RANK, cols), F32),
            tiles(n),
            tiles(pieces, t1),
            tiles(pieces, t1),
            tiles(pieces, t1),
            tiles(n, t1),
            tiles(n, t1),
            tiles(n, zn * t3),
            tiles(n, zn * t3),
            tiles(n, zn, t3),
            tiles(n, zn, t3),
            tiles(far, 2 * t3),
            tiles(2 * t3),
            tiles(n, zn * t3),
            tiles(n, zn * t3),
            tiles(2 * pieces, t1),
            tiles(2),
            tiles(n, zn),
            tiles(far),
            pltpu.SemaphoreType.DMA((4, 3)),
            pltpu.SemaphoreType.DMA((total,)),
            pltpu.SemaphoreType.DMA((total,)),
            pltpu.SemaphoreType.REGULAR((2,)),
        ],
        compiler_params=pltpu.CompilerParams(
            collective_id=0, has_side_effects=True, vmem_limit_bytes=GRANT * 1024
        ),
        name="powersgd",
    )(grad[0], error[0], q_init.T)
    whole, rounded = pl.pallas_call(
        write_out,
        out_shape=(
            jax.ShapeDtypeStruct((rows, cols), F32),
            jax.ShapeDtypeStruct((rows, cols), BF16),
        ),
        in_specs=[vmem] * (parts + 1),
        out_specs=(hbm, hbm),
        scratch_shapes=[pltpu.SemaphoreType.DMA((parts + 1,))],
        compiler_params=pltpu.CompilerParams(vmem_limit_bytes=1024 * 1024),
        name="write_out",
    )(*update, new_error)
    return whole, rounded[None]


def solution(mesh):
    n, z = mesh.shape["dp"], mesh.shape["fsdp"] // (2 * mesh.shape["dp"])
    zn = min(4, z // 2)
    split = Mesh(mesh.devices.reshape(n, z, n, 2), ("dp", *FSDP))
    placed = (P("dp", FSDP, None), P("dp", FSDP, None), P())
    return jax.shard_map(
        functools.partial(body, n, zn, z // zn),
        mesh=split,
        in_specs=placed,
        out_specs=(P(FSDP, None), P("dp", FSDP, None)),
        check_vma=False,
    )
```

```python
import functools

import jax
import jax.numpy as jnp
from jax import lax
from jax.experimental import pallas as pl
from jax.experimental.pallas import tpu as pltpu
from jax.sharding import Mesh
from jax.sharding import PartitionSpec as P

FSDP = ("fsdp_0", "fsdp_1", "fsdp_2")
F32 = jnp.float32
BF16 = jnp.bfloat16
MESH = pl.DeviceIdType.MESH
HIGHEST = lax.Precision.HIGHEST
RANK = 32
PARTS = 4
GRANT = 52200


def three_parts(v):
    hi = v.astype(BF16)
    rest = v - hi.astype(F32)
    mid = rest.astype(BF16)
    return hi, mid, (rest - mid.astype(F32)).astype(BF16)


def far_first(n):
    return sorted(range(1, n), key=lambda k: -min(k, n - k))


def pack(v):
    tile = v[0:8]
    for a in range(1, RANK // 8):
        tile = tile + pltpu.roll(v[8 * a : 8 * a + 8], RANK * a, 1)
    return tile


def unpack(tile):
    spread = [tile] + [pltpu.roll(tile, 128 - RANK * a, 1) for a in range(1, RANK // 8)]
    lane = lax.broadcasted_iota(jnp.int32, (RANK, 128), 1)
    return jnp.where(lane < RANK, jnp.concatenate(spread, axis=0), 0.0)


def kernel(
    dims, g_hbm, e_hbm, q_hbm, *refs
):
    n, zn, far, base, parts = dims
    update_refs, error_ref, refs = refs[:parts], refs[parts], refs[parts + 1 :]
    (
        ge, q0, pslots, core_out, mine, core_in,
        a1, b1, a1s, b1s, a2, b2, f1, zfin, afin, bfin, qfin,
        gcore, gx, gf, load_sem, send, recv, hand,
    ) = refs
    pieces = 2 * n
    y, z = lax.axis_index("dp"), lax.axis_index("fsdp_0")
    x, c = lax.axis_index("fsdp_1"), lax.axis_index("fsdp_2")
    zc, zi = z // zn, z % zn
    rows = g_hbm.shape[0]
    cols = g_hbm.shape[1]
    width = cols // (2 * pieces)
    lanes = width // 128
    t1 = mine.shape[1]
    t2 = t1 // n
    t3 = a2.shape[2]
    sends = []
    sent = iter(range(send.shape[0]))

    def at(dy=0, dx=0, dc=0, dz=0, df=0):
        to_y = (y + dy) % n if dy else y
        to_x = (x + dx) % n if dx else x
        to_c = (c + dc) % 2 if dc else c
        to_zi = (zi + dz) % zn if dz else zi
        to_zc = (zc + df) % far if df else zc
        return (to_y, to_zc * zn + to_zi, to_x, to_c)

    def push(name, src, dst, slot, peer):
        copy = pltpu.make_async_remote_copy(
            src_ref=src, dst_ref=dst,
            send_sem=send.at[next(sent)], recv_sem=recv.at[base[name] + slot],
            device_id=peer, device_id_type=MESH,
        )
        copy.start()
        sends.append(copy)

    def arrive(name, dst, slot):
        pltpu.make_async_remote_copy(
            src_ref=dst, dst_ref=dst,
            send_sem=send.at[0], recv_sem=recv.at[base[name] + slot],
            device_id=at(dc=1), device_id_type=MESH,
        ).wait_recv()

    def arrive_all(name, slots, me, count):
        for k in range(1, count):
            src = (me + k) % count
            arrive(name, slots.at[src], src)

    groups = 4
    step = cols // groups
    loads = []
    for i in range(groups):
        part = pl.ds(i * step, step)
        trio = (
            (g_hbm.at[:, part], ge.at[0:rows, part]),
            (e_hbm.at[:, part], ge.at[rows : 2 * rows, part]),
            (q_hbm.at[:, part], q0.at[:, part]),
        )
        trio = [pltpu.make_async_copy(s, d, load_sem.at[i, j]) for j, (s, d) in enumerate(trio)]
        for copy in trio:
            copy.start()
        loads.append(trio)
    barrier = pltpu.get_barrier_semaphore()
    beside = sorted({1, far - 1})
    near = [at(dy=k, dz=m) for m in range(zn) for k in range(n) if k or m]
    near += [at(dx=k, dz=m) for m in range(zn) for k in range(1, n)]
    near += [at(dc=1)]
    first, last = zi == 0, zi == zn - 1
    below = (y, (z + zn * far - 1) % (zn * far), x, c)
    above = (y, (z + 1) % (zn * far), x, c)

    def tell(sem, peer):
        pl.semaphore_signal(sem, inc=1, device_id=peer, device_id_type=MESH)

    @pl.when(first)
    def _():
        tell(barrier, below)

    @pl.when(last)
    def _():
        tell(barrier, above)

    for peer in near:
        tell(barrier, peer)

    for k in range(n if zn * t3 > t2 else 0):
        a1s[k, t2:] = jnp.zeros((zn * t3 - t2, 8, 128), F32)
        b1s[k, t2:] = jnp.zeros((zn * t3 - t2, 8, 128), F32)

    acc = jnp.zeros((2 * rows, 128), F32)
    sub = step // 2
    for i in range(groups):
        for copy in loads[i]:
            copy.wait()
        for j in range(i * step, (i + 1) * step, sub):
            q = [*three_parts(q0[:, j : j + sub]), jnp.zeros((RANK, sub), BF16)]
            acc = acc + lax.dot_general(
                ge[:, j : j + sub], jnp.concatenate(q, axis=0),
                (((1,), (1,)), ((), ())), preferred_element_type=F32,
            )
    lane = lax.broadcasted_iota(jnp.int32, (rows, 128), 1)
    own = acc[:rows] + acc[rows:]
    own = own + pltpu.roll(own, 96, 1) + pltpu.roll(own, 64, 1)
    pslots[y] = pack(jnp.where(lane < RANK, own, 0.0))

    edge = jnp.where(first, 1, 0) + jnp.where(last, 1, 0)
    pl.semaphore_wait(barrier, len(near) + edge)

    @pl.when(first)
    def _():
        tell(hand.at[2], below)

    @pl.when(last)
    def _():
        tell(hand.at[2], above)

    for k in far_first(n):
        push("p", pslots.at[y], pslots.at[y], y, at(dy=k))
    arrive_all("p", pslots, y, n)

    @pl.when(first | last)
    def _():
        pl.semaphore_wait(hand.at[2], 1)
        for k in range(1, zn):
            tell(hand.at[3], at(dz=k))

    p = pslots[0]
    for k in range(1, n):
        p = p + pslots[k]
    p = unpack(p)

    square = jnp.concatenate([p, jnp.zeros((128 - rows, 128), F32)], axis=0)
    turned = square.T[:RANK]
    gram = lax.dot_general(
        turned, square, (((1,), (0,)), ((), ())), precision=HIGHEST, preferred_element_type=F32
    )
    gcore[c] = pack(gram)
    push("gc", gcore.at[c], gcore.at[c], c, at(dc=1))

    twice = turned + pltpu.roll(turned, rows, 1)
    p3 = jnp.concatenate([*three_parts(twice)], axis=0)[:, : 2 * rows]

    def right(half, piece):
        off = pl.multiple_of((half * pieces + piece) * width, 128)
        r = lax.dot_general(
            p3, ge[:, pl.ds(off, width)], (((1,), (0,)), ((), ())), preferred_element_type=F32
        )
        r = r[:RANK] + (r[RANK : 2 * RANK] + r[2 * RANK :])
        return [r[:, 128 * j : 128 * j + 128].reshape(4, 8, 128) for j in range(lanes)]

    order = []
    for k in [*far_first(n), 0]:
        order += [("a", k, (x + k) % n), ("b", k, n + (y + k) % n)]
    turn = [*far_first(n), 0]

    def first_stage(kind, k, piece, group):
        if kind == "a":
            g = (y + group) % n
            part = pl.ds(g * t2, t2)
            push("a1", mine.at[piece, part], a1.at[x, part], x * n + g, at(dx=k))
        else:
            g = (x + group) % n
            part = pl.ds(g * t2, t2)
            push("b1", mine.at[piece, part], b1.at[y, part], y * n + g, at(dy=k))

    ahead = 3
    for s in range(len(order) + ahead):
        if s < len(order):
            piece = order[s][2]
            for j, tile in enumerate(right((c + 1) % 2, piece)):
                core_out[piece, 4 * j : 4 * j + 4] = tile
            push("cr", core_out.at[piece], core_in.at[piece], s, at(dc=1))
        if s == 4:
            arrive("gc", gcore.at[(c + 1) % 2], (c + 1) % 2)
            gx[x, zi] = gcore[0] + gcore[1]
            for k in turn:
                for m in range(zn):
                    if k or m:
                        push("gx", gx.at[x, zi], gx.at[x, zi], x * zn + zi, at(dx=k, dz=m))
            pl.semaphore_wait(hand.at[3], 2 - edge)
            if far > 2:
                for k in beside:
                    tell(hand.at[0], at(df=k))
        if s >= ahead:
            kind, k, piece = order[s - ahead]
            tiles = right(c, piece)
            arrive("cr", core_in.at[piece], s - ahead)
            for j, tile in enumerate(tiles):
                part = slice(4 * j, 4 * j + 4)
                mine[piece, part] = tile + core_in[piece, part]
            if k:
                for group in turn[: n // 2]:
                    first_stage(kind, k, piece, group)
            if s - ahead == 2 * (n - 1) - 1:
                for group in turn[n // 2 :]:
                    for entry in order[: 2 * (n - 1)]:
                        first_stage(*entry, group)

    direct = [k for k in far_first(far) if min(k, far - k) <= 2]

    def relay(name, slots, low, high):
        if far > 4:
            src = (zc + far - 2) % far
            arrive(name, slots.at[src], src)
            push(name, low(src), low(src), src, at(df=2))
            push(name, slots.at[src], slots.at[src], src, at(df=1))
            src = (zc + 2) % far
            arrive(name, slots.at[src], src)
            if high:
                push(name, high(src), high(src), far, at(df=far - 2))
            push(name, slots.at[src], slots.at[src], src, at(df=far - 1))

    def settle(name, slots, low, high):
        for k in range(1, far):
            src = (zc + k) % far
            if far <= 4 or k in (1, 3, far - 3, far - 1):
                arrive(name, slots.at[src], src)
            elif k == far // 2:
                arrive(name, low(src), src)
                if high:
                    arrive(name, high(src), far)

    def gram_far():
        for k in range(n):
            for m in range(zn):
                if k or m:
                    i, j = (x + k) % n, (zi + m) % zn
                    arrive("gx", gx.at[i, j], i * zn + j)
        total = gx[0, 0]
        for i in range(1, n * zn):
            total = total + gx[i // zn, i % zn]
        gf[zc] = total
        if far > 2:
            pl.semaphore_wait(hand.at[0], len(beside))
        for k in direct:
            push("gf", gf.at[zc], gf.at[zc], zc, at(df=k))

    for group in turn:
        if group == turn[n // 2]:
            gram_far()
        for kind in ("a", "b"):
            if kind == "a":
                me, other, slots, sums, piece = x, y, a1, a1s, x
            else:
                me, other, slots, sums, piece = y, x, b1, b1s, n + y
            g = (other + group) % n
            part = pl.ds(g * t2, t2)
            total = mine[piece, part]
            for k in range(1, n):
                src = (me + k) % n
                arrive(kind + "1", slots.at[src, part], src * n + g)
                total = total + slots[src, part]
            sums[g, 0:t2] = total
            for m in range(zn):
                if group == 0 and m == 0:
                    continue
                chunk = sums.at[g, pl.ds(((zi + m) % zn) * t3, t3)]
                slot = other * zn + zi
                if kind == "a":
                    push("a2", chunk, a2.at[y, zi], slot, at(dy=group, dz=m))
                else:
                    push("b2", chunk, b2.at[x, zi], slot, at(dx=group, dz=m))

    own_part = pl.ds(zi * t3, t3)
    for kind in ("a", "b"):
        other, slots, sums = (y, a2, a1s) if kind == "a" else (x, b2, b1s)
        total = sums[other, own_part]
        for group in [0, *far_first(n)[::-1]]:
            for m in range(zn):
                if group == 0 and m == 0:
                    continue
                o, i = (other + group) % n, (zi + m) % zn
                arrive(kind + "2", slots.at[o, i], o * zn + i)
                total = total + slots[o, i]
        if kind == "a":
            f1[zc, 0:t3] = total
        else:
            f1[zc, t3:] = total

    for k in direct:
        push("f1", f1.at[zc], f1.at[zc], zc, at(df=k))
    gram_cut = (lambda src: gf.at[src], None)
    cut = (lambda src: f1.at[src, 0:t3], lambda src: f1.at[src, t3 : 2 * t3])
    relay("gf", gf, *gram_cut)
    relay("f1", f1, *cut)

    settle("gf", gf, *gram_cut)
    g = gf[0]
    for k in range(1, far):
        g = g + gf[k]
    lane = lax.broadcasted_iota(jnp.int32, (RANK, 128), 1)
    line = lax.broadcasted_iota(jnp.int32, (RANK, 128), 0)
    aug = jnp.where(lane == line + RANK, 1.0, unpack(g))
    for k in range(RANK):
        inv = 1.0 / jnp.sqrt(aug[k : k + 1, k : k + 1])
        row = aug[k : k + 1, :] * inv
        col = aug[:, k : k + 1] * inv
        less = aug - col * row
        aug = jnp.where(line > k, less, jnp.where(line == k, row, aug))
    linv = jnp.where(lane < RANK, pltpu.roll(aug, 96, 1), 0.0)
    linv = jnp.concatenate([linv, jnp.zeros((128 - RANK, 128), F32)], axis=0)
    p_hat = lax.dot_general(
        p, linv, (((1,), (1,)), ((), ())), precision=HIGHEST, preferred_element_type=F32
    )
    w = lax.dot_general(
        p_hat, linv, (((1,), (0,)), ((), ())), precision=HIGHEST, preferred_element_type=F32
    )
    hi, mid, lo = [v.astype(F32) for v in three_parts(w * (1.0 / n))]
    w1 = hi + pltpu.roll(mid, 32, 1) + pltpu.roll(lo, 64, 1) + pltpu.roll(hi, 96, 1)
    w2 = mid + pltpu.roll(hi, 32, 1)
    w6 = jnp.concatenate([w1, w2], axis=1)[:, : 6 * RANK].astype(BF16)

    settle("f1", f1, *cut)
    total = f1[0]
    for k in range(1, far):
        total = total + f1[k]
    zfin[...] = total

    for group in turn[::-1]:
        for m in range(zn):
            if group == 0 and m == 0:
                continue
            slot = zi + zn * y
            push("a3", zfin.at[0:t3], afin.at[y, own_part], slot, at(dy=group, dz=m))
            slot = zi + zn * x
            push("b3", zfin.at[t3 : 2 * t3], bfin.at[x, own_part], slot, at(dx=group, dz=m))
    afin[y, own_part] = total[:t3]
    bfin[x, own_part] = total[t3:]

    def finish(piece):
        q = jnp.concatenate(
            [qfin[piece, 4 * j : 4 * j + 4].reshape(RANK, 128) for j in range(lanes)], axis=1
        )
        hi, mid, lo = three_parts(q)
        q6 = jnp.concatenate([hi, hi, hi, mid, mid, lo], axis=0)
        u = lax.dot_general(w6, q6, (((1,), (0,)), ((), ())), preferred_element_type=F32)
        where = pl.ds(pl.multiple_of(piece * width, 128), width)
        merged = ge[0:rows, where].astype(F32) + ge[rows : 2 * rows, where].astype(F32)
        lines = rows // parts
        for i in range(parts):
            update_refs[i][:, where] = u[i * lines : i * lines + lines]
        error_ref[:, where] = (merged - u).astype(BF16)

    pa, pb = c * pieces + x, c * pieces + n + y
    for group in turn[::-1]:
        for kind in ("a", "b"):
            other, slots, piece = (y, afin, pa) if kind == "a" else (x, bfin, pb)
            g = (other + group) % n
            for m in range(zn):
                if group == 0 and m == 0:
                    continue
                i = (zi + m) % zn
                arrive(kind + "3", slots.at[g, pl.ds(i * t3, t3)], g * zn + i)
            part = pl.ds(g * t2, t2)
            for k in far_first(n):
                if kind == "a":
                    push("a4", afin.at[g, 0:t2], qfin.at[pa, part], x * n + g, at(dx=k))
                else:
                    push("b4", bfin.at[g, 0:t2], qfin.at[pb, part], y * n + g, at(dy=k))
            slot = (0 if kind == "a" else n) + g
            push("cg", slots.at[g, 0:t2], qfin.at[piece, part], slot, at(dc=1))
            qfin[piece, part] = slots[g, 0:t2]

    finish(pa)
    finish(pb)
    half = c * pieces
    turns = []
    for k in far_first(n):
        for name, src, piece in (
            ("a4", (x + n - k) % n, (x + n - k) % n),
            ("b4", (y + n - k) % n, n + (y + n - k) % n),
        ):
            for group in turn[::-1]:
                g = ((y if name == "a4" else x) + group) % n
                arrive(name, qfin.at[half + piece, pl.ds(g * t2, t2)], src * n + g)
            push("ch", qfin.at[half + piece], qfin.at[half + piece], len(turns), at(dc=1))
            turns.append(piece)
            finish(half + piece)
    half = ((c + 1) % 2) * pieces
    for piece, slot in ((x, 0), (n + y, n)):
        for g in range(n):
            arrive("cg", qfin.at[half + piece, g * t2 : g * t2 + t2], slot + g)
        finish(half + piece)
    for s, piece in enumerate(turns):
        arrive("ch", qfin.at[half + piece], s)
        finish(half + piece)
    for copy in sends:
        copy.wait_send()


def write_out(*refs):
    *parts, error, whole, rounded, sem = refs
    lines = parts[0].shape[0]
    copies = [
        pltpu.make_async_copy(part, whole.at[i * lines : i * lines + lines], sem.at[i])
        for i, part in enumerate(parts)
    ]
    copies.append(pltpu.make_async_copy(error, rounded, sem.at[len(parts)]))
    for copy in copies:
        copy.start()
    for copy in copies:
        copy.wait()


def body(n, zn, far, grad, error, q_init):
    rows, cols = grad.shape[1:]
    pieces = 2 * n
    t1 = cols // (2 * pieces) // 128 * (RANK // 8)
    t2 = t1 // n
    t3 = -(-t2 // zn)
    base, total = {}, 0
    for name, count in (
        ("p", n), ("gc", 2), ("gx", n * zn), ("gf", far), ("cr", pieces),
        ("a1", n * n), ("b1", n * n), ("a2", n * zn), ("b2", n * zn), ("f1", far + 1),
        ("a3", n * zn), ("b3", n * zn), ("a4", n * n), ("b4", n * n),
        ("cg", pieces), ("ch", pieces),
    ):
        base[name] = total
        total += count

    def tiles(*lead):
        return pltpu.VMEM((*lead, 8, 128), F32)

    vmem = pl.BlockSpec(memory_space=pltpu.VMEM)
    hbm = pl.BlockSpec(memory_space=pltpu.HBM)
    parts = PARTS
    *update, new_error = pl.pallas_call(
        functools.partial(kernel, (n, zn, far, base, parts)),
        out_shape=(
            *[jax.ShapeDtypeStruct((rows // parts, cols), F32)] * parts,
            jax.ShapeDtypeStruct((rows, cols), BF16),
        ),
        in_specs=[hbm] * 3,
        out_specs=(vmem,) * (parts + 1),
        scratch_shapes=[
            pltpu.VMEM((2 * rows, cols), BF16),
            pltpu.VMEM((RANK, cols), F32),
            tiles(n),
            tiles(pieces, t1),
            tiles(pieces, t1),
            tiles(pieces, t1),
            tiles(n, t1),
            tiles(n, t1),
            tiles(n, zn * t3),
            tiles(n, zn * t3),
            tiles(n, zn, t3),
            tiles(n, zn, t3),
            tiles(far, 2 * t3),
            tiles(2 * t3),
            tiles(n, zn * t3),
            tiles(n, zn * t3),
            tiles(2 * pieces, t1),
            tiles(2),
            tiles(n, zn),
            tiles(far),
            pltpu.SemaphoreType.DMA((4, 3)),
            pltpu.SemaphoreType.DMA((total,)),
            pltpu.SemaphoreType.DMA((total,)),
            pltpu.SemaphoreType.REGULAR((4,)),
        ],
        compiler_params=pltpu.CompilerParams(
            collective_id=0, has_side_effects=True, vmem_limit_bytes=GRANT * 1024
        ),
        name="powersgd",
    )(grad[0], error[0], q_init.T)
    whole, rounded = pl.pallas_call(
        write_out,
        out_shape=(
            jax.ShapeDtypeStruct((rows, cols), F32),
            jax.ShapeDtypeStruct((rows, cols), BF16),
        ),
        in_specs=[vmem] * (parts + 1),
        out_specs=(hbm, hbm),
        scratch_shapes=[pltpu.SemaphoreType.DMA((parts + 1,))],
        compiler_params=pltpu.CompilerParams(vmem_limit_bytes=1024 * 1024),
        name="write_out",
    )(*update, new_error)
    return whole, rounded[None]


def solution(mesh):
    n, z = mesh.shape["dp"], mesh.shape["fsdp"] // (2 * mesh.shape["dp"])
    zn = min(4, z // 2)
    split = Mesh(mesh.devices.reshape(n, z, n, 2), ("dp", *FSDP))
    placed = (P("dp", FSDP, None), P("dp", FSDP, None), P())
    return jax.shard_map(
        functools.partial(body, n, zn, z // zn),
        mesh=split,
        in_specs=placed,
        out_specs=(P(FSDP, None), P("dp", FSDP, None)),
        check_vma=False,
    )
```
